8 devices in a mesh: dp: 1 (over z), tp: 2 (over y), sp: 4 (over x, core).
Axes of the slice: x: 2, y: 2, z: 1, core: 2. Of those that a mesh axis runs over, the one named last changes fastest.
Arguments:
- tok_hidden: bfloat16 [256, 2048], P('dp')
- cache_len: int32 [256], P('dp')
- k_cache: bfloat16 [256, 32, 64, 64], P('dp', 'tp', 'sp')
- v_cache: bfloat16 [256, 32, 64, 64], P('dp', 'tp', 'sp')
- ln_gain: float32 [2048], replicated
- ln_bias: float32 [2048], replicated
- w_qkv: bfloat16 [2048, 3, 32, 64], P(None, None, 'tp')
- b_qkv: bfloat16 [3, 32, 64], P(None, 'tp')
- w_out: bfloat16 [32, 64, 2048], P('tp')
- b_out: bfloat16 [2048], replicated
Outputs:
- output 1: bfloat16 [256, 2048], P('dp')
- output 2: bfloat16 [256, 32, 64, 64], P('dp', 'tp', 'sp')
- output 3: bfloat16 [256, 32, 64, 64], P('dp', 'tp', 'sp')
All inputs are finite; a program needn't handle non-finite values.
Results may differ from the reference program's by a relative error of at most 0.00850116.
Values sent between devices are 32-bit elements.
A program may use at most 1 GiB of HBM per device.

```python
import jax
import jax.numpy as jnp
from jax import lax

BATCH_ROWS = 256
MODEL_DIM = 2048
NUM_HEADS = 32
HEAD_DIM = 64
MAX_LEN = 64


def setup_inputs(seed: int = 0, part: int = 0) -> dict:
    shared_key, part_root = jax.random.split(jax.random.key(seed))
    part_key = jax.random.fold_in(part_root, part)
    part_keys = jax.random.split(part_key, 5)
    shared_keys = jax.random.split(shared_key, 6)
    cache_shape = (BATCH_ROWS, NUM_HEADS, MAX_LEN, HEAD_DIM)
    tok_hidden = 0.5 * jax.random.normal(part_keys[0], (BATCH_ROWS, MODEL_DIM), jnp.float32)
    cache_len = jax.random.randint(part_keys[1], (BATCH_ROWS,), 0, MAX_LEN, jnp.int32)
    cache_len = cache_len.at[0].set(MAX_LEN - 1).at[1].set(0)
    k_cache = 2.0 * jax.random.normal(part_keys[2], cache_shape, jnp.float32)
    coarse = jax.random.normal(part_keys[3], (BATCH_ROWS, NUM_HEADS, 16, HEAD_DIM), jnp.float32)
    v_cache = jnp.repeat(coarse, MAX_LEN // 16, axis=2) + 0.7 * jax.random.normal(part_keys[4], cache_shape, jnp.float32)
    ln_gain = 1.0 + 0.2 * jax.random.normal(shared_keys[0], (MODEL_DIM,), jnp.float32)
    ln_bias = 0.2 * jax.random.normal(shared_keys[1], (MODEL_DIM,), jnp.float32)
    w_qkv = jax.random.normal(shared_keys[2], (MODEL_DIM, 3, NUM_HEADS, HEAD_DIM), jnp.float32) * MODEL_DIM ** -0.5
    b_qkv = 0.3 * jax.random.normal(shared_keys[3], (3, NUM_HEADS, HEAD_DIM), jnp.float32)
    w_out = jax.random.normal(shared_keys[4], (NUM_HEADS, HEAD_DIM, MODEL_DIM), jnp.float32) * (NUM_HEADS * HEAD_DIM) ** -0.5
    b_out = 0.3 * jax.random.normal(shared_keys[5], (MODEL_DIM,), jnp.float32)
    return {
        'tok_hidden': tok_hidden.astype(jnp.bfloat16),
        'cache_len': cache_len,
        'k_cache': k_cache.astype(jnp.bfloat16),
        'v_cache': v_cache.astype(jnp.bfloat16),
        'ln_gain': ln_gain,
        'ln_bias': ln_bias,
        'w_qkv': w_qkv.astype(jnp.bfloat16),
        'b_qkv': b_qkv.astype(jnp.bfloat16),
        'w_out': w_out.astype(jnp.bfloat16),
        'b_out': b_out.astype(jnp.bfloat16),
    }


def reference(tok_hidden, cache_len, k_cache, v_cache, ln_gain, ln_bias, w_qkv, b_qkv, w_out, b_out):
    x_f32 = tok_hidden.astype(jnp.float32)
    mean_x = jnp.mean(x_f32, axis=-1, keepdims=True)
    centered = x_f32 - mean_x
    var_x = jnp.mean(centered * centered, axis=-1, keepdims=True)
    hidden = (centered * lax.rsqrt(var_x + 1e-5) * ln_gain + ln_bias).astype(jnp.bfloat16)
    qkv_flat = jnp.dot(hidden, w_qkv.reshape(MODEL_DIM, 3 * NUM_HEADS * HEAD_DIM), preferred_element_type=jnp.float32)
    qkv_all = (qkv_flat + b_qkv.reshape(3 * NUM_HEADS * HEAD_DIM).astype(jnp.float32)).astype(jnp.bfloat16)
    qkv_all = qkv_all.reshape(BATCH_ROWS, 3, NUM_HEADS, HEAD_DIM)
    q_new = qkv_all[:, 0]
    k_new = qkv_all[:, 1]
    v_new = qkv_all[:, 2]
    slots = jnp.arange(MAX_LEN, dtype=jnp.int32)
    write_mask = (slots[None, :] == cache_len[:, None])[:, None, :, None]
    k_out = jnp.where(write_mask, k_new[:, :, None, :], k_cache)
    v_out = jnp.where(write_mask, v_new[:, :, None, :], v_cache)

    def one_row(row_args):
        q_row, k_row, v_row, row_len = row_args
        scores = jnp.einsum('hd,hsd->hs', q_row.astype(jnp.float32), k_row.astype(jnp.float32)) * HEAD_DIM ** -0.5
        valid = slots[None, :] <= row_len
        prob_w = jax.nn.softmax(jnp.where(valid, scores, -jnp.inf), axis=-1)
        prob_w = prob_w.astype(jnp.bfloat16).astype(jnp.float32)
        return jnp.einsum('hs,hsd->hd', prob_w, v_row.astype(jnp.float32))

    attended = lax.map(one_row, (q_new, k_out, v_out, cache_len))
    projected = jnp.dot(attended.astype(jnp.bfloat16).reshape(BATCH_ROWS, NUM_HEADS * HEAD_DIM), w_out.reshape(NUM_HEADS * HEAD_DIM, MODEL_DIM), preferred_element_type=jnp.float32)
    y_out = (x_f32 + projected + b_out.astype(jnp.float32)).astype(jnp.bfloat16)
    return y_out, k_out, v_out
```

```python
import functools
import jax
import jax.numpy as jnp
from jax import lax
from jax.experimental import pallas as pl
from jax.experimental.pallas import tpu as pltpu
from jax.sharding import PartitionSpec as P

F32 = jnp.float32
BF16 = jnp.bfloat16
GROUP = 4


def attend_kernel(x_hbm, len_hbm, gain_hbm, bias_hbm, bqkv_hbm, w_hbm, k_hbm, v_hbm,
                  k_hbm_out, v_hbm_out, acc_out, max_out, sum_out,
                  k_out, v_out, x_buf, len_ref, gain_ref, bias_ref, bqkv_ref, hidden, w_buf, qkv, bias_cols, x_sem, w_sem, k_sem, v_sem, k_out_sem, v_out_sem):
    heads, slots, dim, rows = k_out.shape
    groups = heads // GROUP
    small = [pltpu.make_async_copy(a, b, x_sem.at[n]) for n, (a, b) in enumerate((
        (x_hbm, x_buf), (len_hbm, len_ref), (gain_hbm, gain_ref), (bias_hbm, bias_ref), (bqkv_hbm, bqkv_ref)))]
    for copy in small:
        copy.start()

    def copy_w(g):
        return pltpu.make_async_copy(w_hbm.at[:, pl.ds(g * GROUP, GROUP)], w_buf.at[:, pl.ds(g * GROUP, GROUP)], w_sem.at[g])

    def copy_k(h):
        return pltpu.make_async_copy(k_hbm.at[h], k_out.at[h], k_sem.at[h])

    def copy_v(h):
        return pltpu.make_async_copy(v_hbm.at[h], v_out.at[h], v_sem.at[h])

    def write_k(h):
        return pltpu.make_async_copy(k_out.at[h], k_hbm_out.at[h], k_out_sem.at[h])

    def write_v(h):
        return pltpu.make_async_copy(v_out.at[h], v_hbm_out.at[h], v_out_sem.at[h])

    for g in range(groups):
        copy_w(g).start()
        for h in range(g * GROUP, (g + 1) * GROUP):
            copy_k(h).start()
            copy_v(h).start()

    for copy in small[1:]:
        copy.wait()
    bias_t = bqkv_ref[...].astype(F32).T
    for j in range(3 * heads):
        bias_cols[j] = jnp.broadcast_to(bias_t[:, j:j + 1], (dim, 128))

    small[0].wait()
    chunk = 16

    @pl.loop(0, rows // chunk)
    def _(i):
        at = pl.ds(pl.multiple_of(i * chunk, chunk), chunk)
        x = x_buf[at, :].astype(F32)
        mean = jnp.mean(x, axis=-1, keepdims=True)
        centered = x - mean
        var = jnp.mean(centered * centered, axis=-1, keepdims=True)
        hidden[at, :] = (centered * lax.rsqrt(var + 1e-5) * gain_ref[...] + bias_ref[...]).astype(BF16)

    local_len = len_ref[...] - lax.axis_index('sp') * slots
    head_id = lax.broadcasted_iota(jnp.int32, (heads, 128), 0)
    max_out[...] = jnp.zeros(max_out.shape, F32)
    sum_out[...] = jnp.zeros(sum_out.shape, F32)
    slot = lax.broadcasted_iota(jnp.int32, (slots, 128), 0)

    @pl.loop(0, groups)
    def _(g):
        copy_w(g).wait()
        w = w_buf[:, pl.ds(g * GROUP, GROUP)].reshape(3 * GROUP * dim, w_buf.shape[-1])
        out = lax.dot_general(w, hidden[...], (((1,), (1,)), ((), ())), preferred_element_type=F32)
        qkv[...] = out.reshape(3, GROUP, dim, rows)

        @pl.loop(0, GROUP)
        def _(i):
            h = g * GROUP + i
            copy_k(h).wait()
            copy_v(h).wait()
            for lane in range(rows // 128):
                b = slice(lane * 128, (lane + 1) * 128)
                here = local_len[:, b]
                q_new = (qkv[0, i, :, b] + bias_cols[h]).astype(BF16).astype(F32)
                k_new = (qkv[1, i, :, b] + bias_cols[heads + h]).astype(BF16)
                v_new = (qkv[2, i, :, b] + bias_cols[2 * heads + h]).astype(BF16)
                parts = []
                for s in range(slots):
                    k = jnp.where(here == s, k_new, k_out[h, s, :, b])
                    k_out[h, s, :, b] = k
                    parts.append(jnp.sum(q_new * k.astype(F32), axis=0, keepdims=True))
                scores = jnp.concatenate(parts, axis=0) * dim ** -0.5
                valid = slot <= here
                masked = jnp.where(valid, scores, -1e30)
                top = jnp.max(masked, axis=0, keepdims=True)
                weights = jnp.where(valid, jnp.exp(masked - top), 0.0)
                max_out[:, b] = jnp.where(head_id == h, top, max_out[:, b])
                sum_out[:, b] = jnp.where(head_id == h, jnp.sum(weights, axis=0, keepdims=True), sum_out[:, b])
                weights = weights.astype(BF16).astype(F32)
                acc = jnp.zeros((dim, 128), F32)
                for s in range(slots):
                    v = jnp.where(here == s, v_new, v_out[h, s, :, b])
                    v_out[h, s, :, b] = v
                    acc = acc + weights[s:s + 1, :] * v.astype(F32)
                acc_out[h, :, b] = acc
            write_k(h).start()
            write_v(h).start()

    @pl.loop(0, heads)
    def _(h):
        write_k(h).wait()
        write_v(h).wait()


def attend(x, cache_len, k, v, gain, bias, w, b):
    heads, slots, dim, rows = k.shape
    model = x.shape[1]
    hbm = pl.BlockSpec(memory_space=pltpu.HBM)
    vmem = pl.BlockSpec(memory_space=pltpu.VMEM)
    return pl.pallas_call(
        attend_kernel,
        out_shape=(
            jax.ShapeDtypeStruct(k.shape, BF16), jax.ShapeDtypeStruct(v.shape, BF16),
            jax.ShapeDtypeStruct((heads, dim, rows), F32), jax.ShapeDtypeStruct((heads, rows), F32), jax.ShapeDtypeStruct((heads, rows), F32),
        ),
        in_specs=[hbm] * 8,
        out_specs=(hbm, hbm, vmem, vmem, vmem),
        scratch_shapes=[
            pltpu.VMEM(k.shape, BF16), pltpu.VMEM(v.shape, BF16),
            pltpu.VMEM((rows, model), BF16), pltpu.VMEM((1, rows), jnp.int32),
            pltpu.VMEM((1, model), F32), pltpu.VMEM((1, model), F32), pltpu.VMEM((3 * heads, dim), BF16),
            pltpu.VMEM((rows, model), BF16),
            pltpu.VMEM((3, heads, dim, model), BF16), pltpu.VMEM((3, GROUP, dim, rows), F32),
            pltpu.VMEM((3 * heads, dim, 128), F32),
            pltpu.SemaphoreType.DMA((5,)), pltpu.SemaphoreType.DMA((heads // GROUP,)),
            pltpu.SemaphoreType.DMA((heads,)), pltpu.SemaphoreType.DMA((heads,)),
            pltpu.SemaphoreType.DMA((heads,)), pltpu.SemaphoreType.DMA((heads,)),
        ],
        compiler_params=pltpu.CompilerParams(vmem_limit_bytes=48 << 20),
        name='attend',
    )(x, cache_len.reshape(1, rows), gain.reshape(1, model), bias.reshape(1, model), b, w, k, v)


CHUNKS = 8
PAIRS = 4


def combine_kernel(acc_ref, max_ref, sum_ref, x_hbm, b_hbm, w_hbm, y_ref,
                   core_acc, core_stat, mix, mix_stat, side_acc, side_stat, att, att_t,
                   x_buf, b_buf, w_buf, part, part_in, final, final_core, final_side, final_relay,
                   in_sem, stat_send, stat_recv, core_send, core_recv, side_send, side_recv, att_send, att_recv,
                   part_send, part_recv, fc_send, fc_recv, fs_send, fs_recv, fr_send, fr_recv):
    heads, dim, rows = acc_ref.shape
    tile = 128
    half_heads = heads // 2
    pair = half_heads // PAIRS
    cols = w_buf.shape[1]
    width = cols // CHUNKS
    tp, sp = lax.axis_index('tp'), lax.axis_index('sp')
    core, side = sp % 2, sp // 2
    dp = lax.axis_index('dp')
    core_peer = (dp, tp, sp + 1 - 2 * core)
    side_peer = (dp, tp, (sp + 2) % 4)
    tp_peer = (dp, 1 - tp, sp)

    def remote(src, dst, send, recv, peer):
        return pltpu.make_async_remote_copy(src_ref=src, dst_ref=dst, send_sem=send, recv_sem=recv,
                                            device_id=peer, device_id_type=pl.DeviceIdType.MESH)

    col0 = pl.multiple_of(core * cols, 128)
    row0 = pl.multiple_of(side * tile, 128)
    other_row0 = pl.multiple_of((1 - side) * tile, 128)
    loads = [pltpu.make_async_copy(w_hbm.at[:, pl.ds(col0, cols)], w_buf, in_sem.at[0]),
             pltpu.make_async_copy(x_hbm.at[pl.ds(row0, tile), pl.ds(col0, cols)], x_buf, in_sem.at[1]),
             pltpu.make_async_copy(b_hbm.at[:, pl.ds(col0, cols)], b_buf, in_sem.at[2])]
    for copy in loads:
        copy.start()

    barrier = pltpu.get_barrier_semaphore()
    for peer in (core_peer, side_peer, tp_peer):
        pl.semaphore_signal(barrier, inc=1, device_id=peer, device_id_type=pl.DeviceIdType.MESH)
    pl.semaphore_wait(barrier, 3)

    mine = pl.multiple_of(core * half_heads, half_heads)
    theirs = pl.multiple_of((1 - core) * half_heads, half_heads)
    stat_copies = [remote(src.at[pl.ds(theirs, half_heads)], core_stat.at[n], stat_send.at[n], stat_recv.at[n], core_peer)
                   for n, src in enumerate((max_ref, sum_ref))]
    core_copies = [remote(acc_ref.at[pl.ds(theirs + j * pair, pair)], core_acc.at[pl.ds(j * pair, pair)],
                          core_send.at[j], core_recv.at[j], core_peer) for j in range(PAIRS)]
    for copy in stat_copies + core_copies:
        copy.start()
    for copy in stat_copies:
        copy.wait_recv()
    own_max, own_sum = max_ref[pl.ds(mine, half_heads)], sum_ref[pl.ds(mine, half_heads)]
    top = jnp.maximum(own_max, core_stat[0])
    own_f, core_f = jnp.exp(own_max - top), jnp.exp(core_stat[0] - top)
    mix_stat[0] = top
    mix_stat[1] = own_sum * own_f + core_stat[1] * core_f
    side_stat_copy = remote(mix_stat.at[:, :, pl.ds(other_row0, tile)], side_stat, stat_send.at[2], stat_recv.at[2], side_peer)
    side_stat_copy.start()
    side_copies = [remote(mix.at[pl.ds(j * pair, pair), :, pl.ds(other_row0, tile)], side_acc.at[pl.ds(j * pair, pair)],
                          side_send.at[j], side_recv.at[j], side_peer) for j in range(PAIRS)]
    for j in range(PAIRS):
        core_copies[j].wait_recv()
        for i in range(j * pair, (j + 1) * pair):
            mix[i] = acc_ref[mine + i] * own_f[i:i + 1, :] + core_acc[i] * core_f[i:i + 1, :]
        side_copies[j].start()

    side_stat_copy.wait_recv()
    my_rows = pl.ds(row0, tile)
    own_max = mix_stat[0, :, my_rows]
    top = jnp.maximum(own_max, side_stat[0])
    own_f, side_f = jnp.exp(own_max - top), jnp.exp(side_stat[0] - top)
    total = mix_stat[1, :, my_rows] * own_f + side_stat[1] * side_f
    att_copies = [remote(att.at[pl.ds(mine + j * pair, pair)], att.at[pl.ds(mine + j * pair, pair)],
                         att_send.at[j], att_recv.at[j], core_peer) for j in range(PAIRS)]
    for j in range(PAIRS):
        side_copies[j].wait_recv()
        for i in range(j * pair, (j + 1) * pair):
            blend = mix[i, :, my_rows] * own_f[i:i + 1, :] + side_acc[i] * side_f[i:i + 1, :]
            att[mine + i] = (blend / total[i:i + 1, :]).astype(BF16).astype(F32)
        att_copies[j].start()
    for copy in att_copies:
        copy.wait_recv()
    for copy in loads:
        copy.wait()
    att_t[...] = att[...].reshape(heads * dim, tile).T.astype(BF16)

    part_copies = [remote(part.at[n], part_in.at[n], part_send.at[n], part_recv.at[n], tp_peer) for n in range(CHUNKS)]
    fc_copies = [remote(final.at[n], final_core.at[n], fc_send.at[n], fc_recv.at[n], core_peer) for n in range(CHUNKS)]
    fs_copies = [remote(final.at[n], final_side.at[n], fs_send.at[n], fs_recv.at[n], side_peer) for n in range(CHUNKS)]
    fr_copies = [remote(final_side.at[n], final_relay.at[n], fr_send.at[n], fr_recv.at[n], core_peer) for n in range(CHUNKS)]
    for n in range(CHUNKS):
        part[n] = jnp.dot(att_t[...], w_buf[:, n * width:(n + 1) * width], preferred_element_type=F32)
        part_copies[n].start()

    other_col0 = pl.multiple_of((1 - core) * cols, 128)

    def put(first_row, first_col, n, value):
        y_ref[pl.ds(first_row, tile), pl.ds(pl.multiple_of(first_col + n * width, 128), width)] = value.astype(BF16)

    def finish(n):
        part_copies[n].wait_recv()
        at = slice(n * width, (n + 1) * width)
        out = x_buf[:, at].astype(F32) + (part[n] + part_in[n]) + b_buf[:, at].astype(F32)
        final[n] = out
        fs_copies[n].start()
        fc_copies[n].start()
        put(row0, col0, n, out)

    def take_core(n):
        fc_copies[n].wait_recv()
        put(row0, other_col0, n, final_core[n])

    def take_side(n):
        fs_copies[n].wait_recv()
        fr_copies[n].start()
        put(other_row0, col0, n, final_side[n])

    def take_relay(n):
        fr_copies[n].wait_recv()
        put(other_row0, other_col0, n, final_relay[n])

    for n in range(CHUNKS + 4):
        if n < CHUNKS:
            finish(n)
        if 1 <= n < CHUNKS + 1:
            take_core(n - 1)
        if 2 <= n < CHUNKS + 2:
            take_side(n - 2)
        if 3 <= n < CHUNKS + 3:
            take_relay(n - 3)
    for copy in (stat_copies + [side_stat_copy] + core_copies + side_copies + att_copies
                 + part_copies + fc_copies + fs_copies + fr_copies):
        copy.wait_send()


def combine(acc, top, total, x, b, w):
    heads, dim, rows = acc.shape
    model = x.shape[1]
    cols = model // 2
    half = heads // 2
    tile = 128
    hbm = pl.BlockSpec(memory_space=pltpu.HBM)
    vmem = pl.BlockSpec(memory_space=pltpu.VMEM)
    dma = pltpu.SemaphoreType.DMA
    block = pltpu.VMEM((CHUNKS, tile, cols // CHUNKS), F32)
    return pl.pallas_call(
        combine_kernel,
        out_shape=jax.ShapeDtypeStruct((rows, model), BF16),
        in_specs=[vmem, vmem, vmem, hbm, hbm, hbm],
        out_specs=vmem,
        scratch_shapes=[
            pltpu.VMEM((half, dim, rows), F32), pltpu.VMEM((2, half, rows), F32),
            pltpu.VMEM((half, dim, rows), F32), pltpu.VMEM((2, half, rows), F32),
            pltpu.VMEM((half, dim, tile), F32), pltpu.VMEM((2, half, tile), F32),
            pltpu.VMEM((heads, dim, tile), F32), pltpu.VMEM((tile, heads * dim), BF16),
            pltpu.VMEM((tile, cols), BF16), pltpu.VMEM((1, cols), BF16), pltpu.VMEM((heads * dim, cols), BF16),
            block, block, block, block, block, block,
            dma((3,)), dma((3,)), dma((3,)), dma((PAIRS,)), dma((PAIRS,)), dma((PAIRS,)), dma((PAIRS,)),
            dma((PAIRS,)), dma((PAIRS,)),
        ] + [dma((CHUNKS,))] * 8,
        compiler_params=pltpu.CompilerParams(vmem_limit_bytes=24 << 20, collective_id=0, has_side_effects=True),
        name='combine',
    )(acc, top, total, x, b.reshape(1, model), w.reshape(heads * dim, model))


def solution(mesh):
    cache_spec = P('dp', 'tp', 'sp', None)
    row_spec = P('dp', None)

    def local_block(tok_hidden, cache_len, k_cache, v_cache, ln_gain, ln_bias, w_qkv, b_qkv, w_out, b_out):
        heads, dim = k_cache.shape[1], k_cache.shape[3]
        k_t, v_t = (c.transpose(1, 2, 3, 0) for c in (k_cache, v_cache))
        k_new, v_new, acc, top, total = attend(
            tok_hidden, cache_len, k_t, v_t, ln_gain, ln_bias, w_qkv.transpose(1, 2, 3, 0), b_qkv.reshape(3 * heads, dim))
        y_out = combine(acc, top, total, tok_hidden, b_out, w_out)
        return y_out, k_new.transpose(3, 0, 1, 2), v_new.transpose(3, 0, 1, 2)

    return jax.shard_map(
        local_block,
        mesh=mesh,
        in_specs=(row_spec, P('dp'), cache_spec, cache_spec, P(None), P(None), P(None, None, 'tp', None), P(None, 'tp', None), P('tp', None, None), P(None)),
        out_specs=(row_spec, cache_spec, cache_spec),
        check_vma=False,
    )
```
